32 devices in a mesh: ta: 2 (over x), gz: 4 (over y, core), gy: 4 (over z).
Axes of the slice: x: 2, y: 2, z: 4, core: 2. Of those that a mesh axis runs over, the one named last changes fastest.
Arguments:
- near_null: float32 [8, 16, 16, 12, 12, 128], P('ta', 'gz', 'gy'), may hold values from -400 to 400
- offsets: int32 [4], replicated, may hold values from 1 to 3
- owner_slot: int32 [2, 4, 4, 16], P('ta', 'gz', 'gy'), may hold values from 0 to 15, each once within a row
Outputs:
- result: float32 [512, 2, 12, 6, 2, 256], P(('ta', 'gz', 'gy'))
The draws below stay inside these ranges and needn't reach their ends.
Inputs may be any that keep to these rules, and one draw needn't show every extreme that they name: The same offsets hold for every device. `owner_slot`: each device's row is a permutation of 0 to 15.
All inputs are finite; a program needn't handle non-finite values.
Results may differ from the reference program's by a relative error of at most 0.0001.
Values sent between devices are 32-bit elements; how exact they have to be, the bound alone decides.
No kernel may reach another device: no remote copies, remote signals or barrier semaphores. Data moves between devices by JAX's collectives and lax.ppermute only.
A program may use at most 256 MiB of HBM per device.

```python
import jax
import jax.numpy as jnp
from jax import lax

V = 12
C = 12
AGG = 4
NX = 64
NT = 8
NZ = 16
NY = 16
NAGG = 16
N_TA = 2
N_GZ = 4
N_GY = 4


def draw_near_null(key, part):
    key_base, key_site, key_vector = jax.random.split(key, 3)
    shape = (NT, NZ, NY, V, C, 2 * NX)
    site_scale = jnp.exp(jax.random.uniform(key_site, (NT, NZ, NY, 1, 1, 2 * NX), jnp.float32) * jnp.log(10.0))
    vector_scale = jnp.exp(jax.random.uniform(key_vector, (1, 1, 1, V, 1, 1), jnp.float32) * jnp.log(10.0))
    base = jnp.clip(jax.random.normal(key_base, shape, jnp.float32), -4.0, 4.0)
    return (base * site_scale * vector_scale).astype(jnp.float32)


def with_ends(entries, rng, smallest, high):
    longest = entries.shape.index(max(entries.shape))
    spots = []
    for shift in (0, 1):
        where = [jax.random.randint(jax.random.fold_in(rng, axis), (), 0, length) for axis, length in enumerate(entries.shape)]
        where[longest] = (where[longest] + shift) % entries.shape[longest]
        spots.append(tuple(where))
    return entries.at[spots[0]].set(smallest).at[spots[1]].set(high)


def setup_inputs(seed: int = 0) -> dict:
    key_of = jax.random.split(jax.random.key(seed), 4)
    near_null = draw_near_null(jax.random.fold_in(key_of[3], 71), 0)
    offsets = with_ends(jax.random.randint(key_of[1], (4,), 1, AGG), jax.random.fold_in(key_of[1], 1), 1, AGG - 1).astype(jnp.int32)
    owner_slot = jax.vmap(lambda own: jax.random.permutation(own, NAGG))(jax.random.split(key_of[2], N_TA * N_GZ * N_GY)).reshape((N_TA, N_GZ, N_GY, NAGG)).astype(jnp.int32)
    return {"near_null": near_null, "offsets": offsets, "owner_slot": owner_slot}


ridge_scale = 0.05
top_precision = lax.Precision.HIGHEST

def factor_pass(blocks):
    norm_count = blocks.shape[3] * blocks.shape[5]
    products = jnp.einsum('nkvcas,nkwcbs->nkavbw', blocks, blocks, precision=top_precision) / norm_count
    gram_real = products[:, :, 0, :, 0, :] + products[:, :, 1, :, 1, :]
    gram_imag = products[:, :, 0, :, 1, :] - products[:, :, 1, :, 0, :]
    width = gram_real.shape[-1]
    diag_mean = lax.optimization_barrier(jnp.mean(jnp.diagonal(gram_real, axis1=2, axis2=3), axis=-1))
    ridge_term = ridge_scale * (diag_mean + 1e-06)
    gram_real = jnp.moveaxis(gram_real, (2, 3), (0, 1))
    gram_imag = jnp.moveaxis(gram_imag, (2, 3), (0, 1))
    zero_batch = jnp.zeros_like(ridge_term)
    low_real = [[zero_batch] * width for row_idx in range(width)]
    low_imag = [[zero_batch] * width for row_idx in range(width)]
    for col_idx in range(width):
        remain = gram_real[col_idx, col_idx] + ridge_term
        for mid_idx in range(col_idx):
            remain = remain - low_real[col_idx][mid_idx] * low_real[col_idx][mid_idx]
            remain = remain - low_imag[col_idx][mid_idx] * low_imag[col_idx][mid_idx]
        diag_val = jnp.sqrt(remain)
        low_real[col_idx][col_idx] = diag_val
        for row_idx in range(col_idx + 1, width):
            sum_real = gram_real[row_idx, col_idx]
            sum_imag = gram_imag[row_idx, col_idx]
            for mid_idx in range(col_idx):
                left_real = low_real[row_idx][mid_idx]
                left_imag = low_imag[row_idx][mid_idx]
                right_real = low_real[col_idx][mid_idx]
                right_imag = low_imag[col_idx][mid_idx]
                sum_real = sum_real - (left_real * right_real + left_imag * right_imag)
                sum_imag = sum_imag - (left_imag * right_real - left_real * right_imag)
            low_real[row_idx][col_idx] = sum_real / diag_val
            low_imag[row_idx][col_idx] = sum_imag / diag_val
    inv_real = [[zero_batch] * width for row_idx in range(width)]
    inv_imag = [[zero_batch] * width for row_idx in range(width)]
    for col_idx in range(width):
        inv_real[col_idx][col_idx] = 1.0 / low_real[col_idx][col_idx]
        for row_idx in range(col_idx + 1, width):
            sum_real = zero_batch
            sum_imag = zero_batch
            for mid_idx in range(col_idx, row_idx):
                left_real = low_real[row_idx][mid_idx]
                left_imag = low_imag[row_idx][mid_idx]
                right_real = inv_real[mid_idx][col_idx]
                right_imag = inv_imag[mid_idx][col_idx]
                sum_real = sum_real + left_real * right_real - left_imag * right_imag
                sum_imag = sum_imag + left_real * right_imag + left_imag * right_real
            inv_real[row_idx][col_idx] = -sum_real / low_real[row_idx][row_idx]
            inv_imag[row_idx][col_idx] = -sum_imag / low_real[row_idx][row_idx]
    map_real = jnp.stack([jnp.stack([inv_real[w_idx][v_idx] for w_idx in range(width)], axis=-1) for v_idx in range(width)], axis=-2)
    map_imag = -jnp.stack([jnp.stack([inv_imag[w_idx][v_idx] for w_idx in range(width)], axis=-1) for v_idx in range(width)], axis=-2)
    mixing = jnp.stack([jnp.stack([map_real, map_imag], axis=3), jnp.stack([-map_imag, map_real], axis=3)], axis=2)
    return jnp.einsum('nkvcas,nkavbw->nkwcbs', blocks, mixing, precision=top_precision)

def two_passes(blocks):
    return factor_pass(factor_pass(blocks))

def reference(near_null, offsets, owner_slot):
    lattice = near_null.reshape(NT, NZ, NY, V, C, 2, NX)
    lattice = jnp.roll(lattice, -offsets[0], axis=0)
    lattice = jnp.roll(lattice, -offsets[1], axis=1)
    lattice = jnp.roll(lattice, -offsets[2], axis=2)
    lattice = jnp.roll(lattice, -offsets[3], axis=6)
    half_c = C // 2
    pieces = lattice.reshape(N_TA, AGG, N_GZ, AGG, N_GY, AGG, V, 2, half_c, 2, NAGG, AGG)
    pieces = pieces.transpose(0, 2, 4, 10, 7, 6, 8, 9, 1, 3, 5, 11)
    site_count = AGG * AGG * AGG * AGG
    device_count = N_TA * N_GZ * N_GY
    flattened = pieces.reshape(device_count * NAGG, 2, V, half_c, 2, site_count)
    source_of = jnp.argsort(owner_slot, axis=-1).astype(jnp.int32)
    device_base = (jnp.arange(device_count, dtype=jnp.int32) * NAGG).reshape(N_TA, N_GZ, N_GY, 1)
    packed = jnp.take(flattened, (device_base + source_of).reshape(-1), axis=0)
    per_peer = NAGG // N_TA
    packed = packed.reshape(N_TA, N_GZ, N_GY, N_TA, per_peer, 2, V, half_c, 2, site_count)
    owned_aggs = packed.transpose(3, 1, 2, 0, 4, 5, 6, 7, 8, 9).reshape(device_count, NAGG, 2, V, half_c, 2, site_count)
    result = lax.map(two_passes, owned_aggs)
    return result.reshape(device_count * NAGG, 2, V, half_c, 2, site_count)
```

```python
import jax
import jax.numpy as jnp
from jax import lax
from jax.experimental import pallas as pl
from jax.experimental.pallas import tpu as pltpu
from jax.sharding import PartitionSpec as P

ridge_scale = 0.05
top = lax.Precision.HIGHEST
LANES = 128
direct_limit = 4


def from_behind(array, axis, by):
    length = lax.axis_size(axis)
    return lax.ppermute(array, axis, [(i, (i + by) % length) for i in range(length)])


def pack(aligned, shift, table, edge):
    rows = aligned.shape[3]
    half = LANES // 2
    sites = edge * edge
    groups = half // edge
    low_bit = edge.bit_length() - 1

    def body(shift_ref, table_ref, in_ref, out_ref):
        row_t = pl.program_id(0)
        move = shift_ref[0]
        lane = lax.broadcasted_iota(jnp.int32, (8, LANES), 1)
        wraps = (lane % half) >= (half - move)

        def step(g, carry):
            at = pl.ds(pl.multiple_of(g * 8, 8), 8)
            regs = []
            for site in range(sites):
                value = in_ref[0, site // edge, site % edge, at, :]
                near = pltpu.roll(value, LANES - move, 1)
                far = pltpu.roll(value, half - move, 1)
                regs.append(jnp.where(wraps, far, near))
            bit = 1
            while bit < sites:
                dist = bit << low_bit
                keep = (lane & dist) == 0
                fresh = list(regs)
                for i in range(sites):
                    if not i & bit:
                        a, b = regs[i], regs[i | bit]
                        fresh[i] = jnp.where(keep, a, pltpu.roll(b, dist, 1))
                        fresh[i | bit] = jnp.where(keep, pltpu.roll(a, LANES - dist, 1), b)
                regs = fresh
                bit *= 2
            for j in range(groups):
                out_ref[table_ref[row_t, j], 0, at, :] = regs[j]
            return carry

        lax.fori_loop(0, rows // 8, step, 0)

    return pl.pallas_call(
        body,
        grid_spec=pltpu.PrefetchScalarGridSpec(
            num_scalar_prefetch=2,
            grid=(edge,),
            in_specs=[pl.BlockSpec((1, edge, edge, rows, LANES), lambda r, s, t: (r, 0, 0, 0, 0))],
            out_specs=pl.BlockSpec((groups, 1, rows, LANES), lambda r, s, t: (0, r, 0, 0)),
        ),
        out_shape=jax.ShapeDtypeStruct((groups, edge, rows, LANES), jnp.float32),
        name="pack",
    )(shift, table, aligned)


def joined(refs):
    half = LANES // 2
    lane = lax.broadcasted_iota(jnp.int32, refs[0].shape[3:], 1)
    low = lane < half
    reals, imags = [], []
    for i in range(0, len(refs), 2):
        a = refs[i][0, 0, 0]
        b = refs[i + 1][0, 0, 0]
        reals.append(jnp.where(low, a, pltpu.roll(b, half, 1)))
        imags.append(jnp.where(low, pltpu.roll(a, half, 1), b))
    return jnp.concatenate(
        [jnp.concatenate(reals, axis=1), jnp.concatenate(imags, axis=1)], axis=0
    )


def block_specs(rows, edge):
    def spec(t):
        return pl.BlockSpec(
            (1, 1, 1, rows, LANES), lambda n, k, p, r: (k[n, t], p[n, t], r[n, t], 0, 0)
        )

    return [spec(t) for t in range(edge)]


def fixed(shape):
    return pl.BlockSpec(shape, lambda n, k, p, r: (0,) * len(shape))


def grams(blocks, where, spread, gather, match, norm_count):
    edge, rows = blocks.shape[2], blocks.shape[3]
    count = where[0].shape[0]
    wide = gather.shape[0]

    def body(k_ref, p_ref, r_ref, *refs):
        spread_ref, gather_ref, match_ref, out_ref = refs[edge:]
        w = joined(refs[:edge])
        full = lax.dot_general(
            w, w, (((1,), (1,)), ((), ())), precision=top, preferred_element_type=jnp.float32
        )
        full = full * match_ref[...]
        part = jnp.dot(full, spread_ref[...], precision=top, preferred_element_type=jnp.float32)
        out_ref[0] = (
            jnp.dot(gather_ref[...], part, precision=top, preferred_element_type=jnp.float32)
            / norm_count
        )

    return pl.pallas_call(
        body,
        grid_spec=pltpu.PrefetchScalarGridSpec(
            num_scalar_prefetch=3,
            grid=(count,),
            in_specs=block_specs(rows, edge)
            + [fixed(spread.shape), fixed(gather.shape), fixed(match.shape)],
            out_specs=pl.BlockSpec((1, wide, wide), lambda n, k, p, r: (n, 0, 0)),
        ),
        out_shape=jax.ShapeDtypeStruct((count, wide, wide), jnp.float32),
        name="gram",
    )(*where, *([blocks] * edge), spread, gather, match)


def apply(blocks, where, mixing, spread, gather, match, chirality, result, chiralities):
    edge, rows = blocks.shape[2], blocks.shape[3]
    count = where[0].shape[0]
    wide = gather.shape[0]
    out_rows = rows * 4

    def body(k_ref, p_ref, r_ref, *refs):
        mix_ref, spread_ref, gather_ref, match_ref = refs[edge : edge + 4]
        out_ref = refs[-1]
        w = joined(refs[:edge])
        part = jnp.dot(
            mix_ref[0], gather_ref[...], precision=top, preferred_element_type=jnp.float32
        )
        full = jnp.dot(spread_ref[...], part, precision=top, preferred_element_type=jnp.float32)
        full = full * match_ref[...]
        out = jnp.dot(full, w, precision=top, preferred_element_type=jnp.float32)
        for ri in range(2):
            for s in range(2):
                out_ref[0, 0, pl.ds(s * 2 + ri, rows, stride=4), :] = out[
                    ri * rows : (ri + 1) * rows, s * LANES : (s + 1) * LANES
                ]

    in_specs = block_specs(rows, edge) + [
        pl.BlockSpec((1, wide, wide), lambda n, k, p, r: (n, 0, 0)),
        fixed(spread.shape),
        fixed(gather.shape),
        fixed(match.shape),
    ]
    operands = [*where, *([blocks] * edge), mixing, spread, gather, match]
    aliases = {}
    if result is not None:
        aliases = {len(operands): 0}
        operands.append(result)
        in_specs.append(pl.BlockSpec(memory_space=pl.ANY))
    return pl.pallas_call(
        body,
        grid_spec=pltpu.PrefetchScalarGridSpec(
            num_scalar_prefetch=3,
            grid=(count,),
            in_specs=in_specs,
            out_specs=pl.BlockSpec(
                (1, 1, out_rows, LANES), lambda n, k, p, r: (n, chirality, 0, 0)
            ),
        ),
        out_shape=jax.ShapeDtypeStruct((count, chiralities, out_rows, LANES), jnp.float32),
        input_output_aliases=aliases,
        name="mix",
    )(*operands)


def inverse_factors(ar, ai):
    width = ar.shape[0]
    row = lax.broadcasted_iota(jnp.int32, ar.shape, 0)
    col = lax.broadcasted_iota(jnp.int32, ar.shape, 1)
    diag = row == col
    eye = jnp.where(diag, 1.0, 0.0)
    mr, mi = eye, jnp.zeros_like(ar)
    tr, ti = eye, jnp.zeros_like(ar)
    for j in range(width):
        inv = 1.0 / ar[j : j + 1, j : j + 1]
        below = row[:, j : j + 1] > j
        fr = jnp.where(below, ar[:, j : j + 1] * inv, 0.0)
        fi = jnp.where(below, ai[:, j : j + 1] * inv, 0.0)
        right = col[j : j + 1] > j
        gr = jnp.where(right, ar[j : j + 1] * inv, 0.0)
        gi = jnp.where(right, -ai[j : j + 1] * inv, 0.0)
        pr, pi = ar[j : j + 1], ai[j : j + 1]
        qr, qi = mr[j : j + 1], mi[j : j + 1]
        ur, ui = tr[:, j : j + 1], ti[:, j : j + 1]
        ar, ai = ar - (fr * pr - fi * pi), ai - (fr * pi + fi * pr)
        mr, mi = mr - (fr * qr - fi * qi), mi - (fr * qi + fi * qr)
        tr, ti = tr - (gr * ur - gi * ui), ti - (gr * ui + gi * ur)
    pivots = jnp.where(diag, ar, 0.0)
    by_row = 1.0 / jnp.sqrt(jnp.sum(pivots, axis=1, keepdims=True))
    by_col = 1.0 / jnp.sqrt(jnp.sum(pivots, axis=0, keepdims=True))
    return mr * by_row, mi * by_row, tr * by_col, ti * by_col


def mixers(gram_real, gram_imag):
    width = gram_real.shape[0]

    def body(gr_ref, gi_ref, kr_ref, ki_ref):
        ar, ai = gr_ref[...], gi_ref[...]
        row = lax.broadcasted_iota(jnp.int32, ar.shape, 0)
        col = lax.broadcasted_iota(jnp.int32, ar.shape, 1)
        diag = row == col

        def ridge_of(real):
            total = jnp.sum(jnp.where(diag, real, 0.0), axis=0, keepdims=True)
            mean = jnp.sum(total, axis=1, keepdims=True) / width
            return ridge_scale * (mean + 1e-06)

        ridge = ridge_of(ar)
        ar = ar + jnp.where(diag, ridge, 0.0)
        mr, mi, tr, ti = inverse_factors(ar, ai)
        xr = jnp.zeros_like(ar)
        xi = jnp.zeros_like(ar)
        for m in range(width):
            lr, li = mr[:, m : m + 1], mi[:, m : m + 1]
            cr, ci = tr[m : m + 1], -ti[m : m + 1]
            xr = xr + (lr * cr - li * ci)
            xi = xi + (lr * ci + li * cr)
        br = jnp.where(diag, 1.0, 0.0) - ridge * xr
        bi = -ridge * xi
        br = br + jnp.where(diag, ridge_of(br), 0.0)
        sr, si, _, _ = inverse_factors(br, bi)
        kr = jnp.zeros_like(ar)
        ki = jnp.zeros_like(ar)
        for m in range(width):
            lr, li = sr[:, m : m + 1], si[:, m : m + 1]
            cr, ci = mr[m : m + 1], mi[m : m + 1]
            kr = kr + (lr * cr - li * ci)
            ki = ki + (lr * ci + li * cr)
        kr_ref[...] = kr
        ki_ref[...] = ki

    shape = jax.ShapeDtypeStruct(gram_real.shape, jnp.float32)
    return pl.pallas_call(body, out_shape=(shape, shape), name="factor")(gram_real, gram_imag)


def per_device(near_null, offsets, owner_slot):
    edge, _, _, vectors, comps, lanes = near_null.shape
    chiralities = 2
    half_c = comps // chiralities
    ta_size = lax.axis_size("ta")
    me = lax.axis_index("ta")
    direct = ta_size <= direct_limit
    slots = owner_slot.reshape(-1)
    count = slots.shape[0]
    per_peer = count // ta_size
    off_t = offsets[0]
    shift = offsets[3:4]

    before = from_behind(slots, "ta", 1)

    def places(slot_row):
        if not direct:
            return slot_row
        return ((slot_row // per_peer - me) % ta_size) * per_peer + slot_row % per_peer

    row_ids = jnp.arange(edge, dtype=jnp.int32)
    table = jnp.where((row_ids >= off_t)[:, None], places(slots)[None], places(before)[None])

    chunks = near_null.reshape(edge, edge, edge, vectors, chiralities, half_c, lanes)
    rows = vectors * half_c
    chunks = tuple(
        chunks[:, :, :, :, h].reshape(edge, edge, edge, rows, lanes) for h in range(chiralities)
    )

    def exchange(packed):
        packed = packed.reshape((ta_size, per_peer) + packed.shape[1:])
        if not direct:
            return lax.all_to_all(packed, "ta", split_axis=0, concat_axis=0, tiled=True)
        parts = [packed[:1]]
        for k in range(1, ta_size):
            parts.append(from_behind(packed[k : k + 1], "ta", k))
        return jnp.concatenate(parts, axis=0)

    def travel(off_z, off_y):
        def run(data):
            results = []
            for d in data:
                corner = from_behind(d[:, :off_z, :off_y], "gz", -1)
                side_y = from_behind(d[:, off_z:, :off_y], "gy", -1)
                side_z = from_behind(d[:, :off_z, off_y:], "gz", -1)
                corner = from_behind(corner, "gy", -1)
                left = jnp.concatenate([d[:, off_z:, off_y:], side_z], axis=1)
                right = jnp.concatenate([side_y, corner], axis=1)
                aligned = jnp.concatenate([left, right], axis=2)
                results.append(exchange(pack(aligned, shift, table, edge)))
            return tuple(results)

        return run

    branches = [travel(i, j) for i in range(1, edge) for j in range(1, edge)]
    chunks = lax.switch((offsets[1] - 1) * (edge - 1) + (offsets[2] - 1), branches, chunks)

    owned = jnp.arange(count, dtype=jnp.int32)
    time_row = ((owned // per_peer) * edge)[:, None] + row_ids[None] + off_t
    time_row = time_row % (edge * ta_size)
    source = time_row // edge
    if direct:
        source = (me - source) % ta_size
    slot = jnp.broadcast_to((owned % per_peer)[:, None], (count, edge))
    where = (source, slot, time_row % edge)

    wide = 2 * vectors
    index = jnp.arange(2 * rows, dtype=jnp.int32)
    spread = (index[:, None] // half_c == jnp.arange(wide)[None]).astype(jnp.float32)
    gather = spread.T
    match = (index[:, None] % half_c == index[None] % half_c).astype(jnp.float32)

    norm_count = half_c * edge**4
    result = None
    for h, blocks in enumerate(chunks):
        gram = grams(blocks, where, spread, gather, match, norm_count)
        gram = gram.reshape(count, 2, vectors, 2, vectors).transpose(1, 3, 2, 4, 0)
        kr, ki = mixers(gram[0, 0] + gram[1, 1], gram[0, 1] - gram[1, 0])
        mixing = jnp.stack([jnp.stack([kr, ki]), jnp.stack([-ki, kr])])
        mixing = mixing.transpose(4, 0, 2, 1, 3).reshape(count, wide, wide)
        result = apply(blocks, where, mixing, spread, gather, match, h, result, chiralities)
    halves = edge**4 // LANES
    result = result.reshape(count, chiralities, vectors, half_c, halves, 2, LANES)
    result = result.transpose(0, 1, 2, 3, 5, 4, 6)
    return result.reshape(count, chiralities, vectors, half_c, 2, edge**4)


def solution(mesh):
    return jax.shard_map(
        per_device,
        mesh=mesh,
        in_specs=(P("ta", "gz", "gy", None, None, None), P(), P("ta", "gz", "gy", None)),
        out_specs=P(("ta", "gz", "gy"), None, None, None, None, None),
        check_vma=False,
    )
```

```python
import jax
import jax.numpy as jnp
from jax import lax
from jax.experimental import pallas as pl
from jax.experimental.pallas import tpu as pltpu
from jax.sharding import PartitionSpec as P

ridge_scale = 0.05
top = lax.Precision.HIGHEST
LANES = 128
direct_limit = 4


def from_behind(array, axis, by):
    length = lax.axis_size(axis)
    return lax.ppermute(array, axis, [(i, (i + by) % length) for i in range(length)])


def pack(aligned, shift, table, edge):
    rows = aligned.shape[3]
    half = LANES // 2
    sites = edge * edge
    groups = half // edge
    low_bit = edge.bit_length() - 1

    def body(shift_ref, table_ref, in_ref, out_ref):
        row_t = pl.program_id(0)
        move = shift_ref[0]
        lane = lax.broadcasted_iota(jnp.int32, (8, LANES), 1)
        wraps = (lane % half) >= (half - move)

        def step(g, carry):
            at = pl.ds(pl.multiple_of(g * 8, 8), 8)
            regs = []
            for site in range(sites):
                value = in_ref[0, site // edge, site % edge, at, :]
                near = pltpu.roll(value, LANES - move, 1)
                far = pltpu.roll(value, half - move, 1)
                regs.append(jnp.where(wraps, far, near))
            bit = 1
            while bit < sites:
                dist = bit << low_bit
                keep = (lane & dist) == 0
                fresh = list(regs)
                for i in range(sites):
                    if not i & bit:
                        a, b = regs[i], regs[i | bit]
                        fresh[i] = jnp.where(keep, a, pltpu.roll(b, dist, 1))
                        fresh[i | bit] = jnp.where(keep, pltpu.roll(a, LANES - dist, 1), b)
                regs = fresh
                bit *= 2
            for j in range(groups):
                out_ref[table_ref[row_t, j], 0, at, :] = regs[j]
            return carry

        lax.fori_loop(0, rows // 8, step, 0, unroll=3 if rows % 24 == 0 else 1)

    return pl.pallas_call(
        body,
        grid_spec=pltpu.PrefetchScalarGridSpec(
            num_scalar_prefetch=2,
            grid=(edge,),
            in_specs=[pl.BlockSpec((1, edge, edge, rows, LANES), lambda r, s, t: (r, 0, 0, 0, 0))],
            out_specs=pl.BlockSpec((groups, 1, rows, LANES), lambda r, s, t: (0, r, 0, 0)),
        ),
        out_shape=jax.ShapeDtypeStruct((groups, edge, rows, LANES), jnp.float32),
        name="pack",
    )(shift, table, aligned)


def joined(refs):
    half = LANES // 2
    lane = lax.broadcasted_iota(jnp.int32, refs[0].shape[3:], 1)
    low = lane < half
    reals, imags = [], []
    for i in range(0, len(refs), 2):
        a = refs[i][0, 0, 0]
        b = refs[i + 1][0, 0, 0]
        reals.append(jnp.where(low, a, pltpu.roll(b, half, 1)))
        imags.append(jnp.where(low, pltpu.roll(a, half, 1), b))
    return jnp.concatenate(
        [jnp.concatenate(reals, axis=1), jnp.concatenate(imags, axis=1)], axis=0
    )


def batch_of(count):
    return 4 if count % 4 == 0 else 1


def block_specs(rows, edge, batch):
    def spec(u, t):
        def index(n, k, p, r):
            at = n * batch + u
            return (k[at, t], p[at, t], r[at, t], 0, 0)

        return pl.BlockSpec((1, 1, 1, rows, LANES), index)

    return [spec(u, t) for u in range(batch) for t in range(edge)]


def fixed(shape):
    return pl.BlockSpec(shape, lambda n, k, p, r: (0,) * len(shape))


def grams(blocks, where, spread, gather, match, norm_count, batch):
    edge, rows = blocks.shape[2], blocks.shape[3]
    count = where[0].shape[0]
    wide = gather.shape[0]

    def body(k_ref, p_ref, r_ref, *refs):
        spread_ref, gather_ref, match_ref, out_ref = refs[edge * batch :]
        fulls = []
        for u in range(batch):
            w = joined(refs[u * edge : (u + 1) * edge])
            full = lax.dot_general(
                w, w, (((1,), (1,)), ((), ())), precision=top, preferred_element_type=jnp.float32
            )
            fulls.append(full * match_ref[...])
        tall = jnp.concatenate(fulls, axis=0)
        part = jnp.dot(tall, spread_ref[...], precision=top, preferred_element_type=jnp.float32)
        size = 2 * rows
        for u in range(batch):
            out_ref[u] = (
                jnp.dot(
                    gather_ref[...],
                    part[u * size : (u + 1) * size],
                    precision=top,
                    preferred_element_type=jnp.float32,
                )
                / norm_count
            )

    return pl.pallas_call(
        body,
        grid_spec=pltpu.PrefetchScalarGridSpec(
            num_scalar_prefetch=3,
            grid=(count // batch,),
            in_specs=block_specs(rows, edge, batch)
            + [fixed(spread.shape), fixed(gather.shape), fixed(match.shape)],
            out_specs=pl.BlockSpec((batch, wide, wide), lambda n, k, p, r: (n, 0, 0)),
        ),
        out_shape=jax.ShapeDtypeStruct((count, wide, wide), jnp.float32),
        name="gram",
    )(*where, *([blocks] * (edge * batch)), spread, gather, match)


def apply(blocks, where, mixing, spread, gather, match, chirality, result, chiralities):
    edge, rows = blocks.shape[2], blocks.shape[3]
    count = where[0].shape[0]
    wide = gather.shape[0]
    out_rows = rows * 4
    batch = batch_of(count)

    def body(k_ref, p_ref, r_ref, *refs):
        mix_ref, spread_ref, gather_ref, match_ref = refs[edge * batch : edge * batch + 4]
        out_ref = refs[-1]
        parts = [
            jnp.dot(mix_ref[u], gather_ref[...], precision=top, preferred_element_type=jnp.float32)
            for u in range(batch)
        ]
        fulls = [
            jnp.dot(spread_ref[...], part, precision=top, preferred_element_type=jnp.float32)
            for part in parts
        ]
        for u in range(batch):
            w = joined(refs[u * edge : (u + 1) * edge])
            full = fulls[u] * match_ref[...]
            out = jnp.dot(full, w, precision=top, preferred_element_type=jnp.float32)
            for ri in range(2):
                for s in range(2):
                    out_ref[u, 0, pl.ds(s * 2 + ri, rows, stride=4), :] = out[
                        ri * rows : (ri + 1) * rows, s * LANES : (s + 1) * LANES
                    ]

    in_specs = block_specs(rows, edge, batch) + [
        pl.BlockSpec((batch, wide, wide), lambda n, k, p, r: (n, 0, 0)),
        fixed(spread.shape),
        fixed(gather.shape),
        fixed(match.shape),
    ]
    operands = [*where, *([blocks] * (edge * batch)), mixing, spread, gather, match]
    aliases = {}
    if result is not None:
        aliases = {len(operands): 0}
        operands.append(result)
        in_specs.append(pl.BlockSpec(memory_space=pl.ANY))
    return pl.pallas_call(
        body,
        grid_spec=pltpu.PrefetchScalarGridSpec(
            num_scalar_prefetch=3,
            grid=(count // batch,),
            in_specs=in_specs,
            out_specs=pl.BlockSpec(
                (batch, 1, out_rows, LANES), lambda n, k, p, r: (n, chirality, 0, 0)
            ),
        ),
        out_shape=jax.ShapeDtypeStruct((count, chiralities, out_rows, LANES), jnp.float32),
        input_output_aliases=aliases,
        name="mix",
    )(*operands)


def inverse_factors(ar, ai):
    width = ar.shape[0]
    row = lax.broadcasted_iota(jnp.int32, ar.shape, 0)
    col = lax.broadcasted_iota(jnp.int32, ar.shape, 1)
    diag = row == col
    eye = jnp.where(diag, 1.0, 0.0)
    mr, mi = eye, jnp.zeros_like(ar)
    tr, ti = eye, jnp.zeros_like(ar)
    for j in range(width):
        inv = 1.0 / ar[j : j + 1, j : j + 1]
        below = row[:, j : j + 1] > j
        fr = jnp.where(below, ar[:, j : j + 1] * inv, 0.0)
        fi = jnp.where(below, ai[:, j : j + 1] * inv, 0.0)
        right = col[j : j + 1] > j
        gr = jnp.where(right, ar[j : j + 1] * inv, 0.0)
        gi = jnp.where(right, -ai[j : j + 1] * inv, 0.0)
        pr, pi = ar[j : j + 1], ai[j : j + 1]
        qr, qi = mr[j : j + 1], mi[j : j + 1]
        ur, ui = tr[:, j : j + 1], ti[:, j : j + 1]
        ar, ai = ar - (fr * pr - fi * pi), ai - (fr * pi + fi * pr)
        mr, mi = mr - (fr * qr - fi * qi), mi - (fr * qi + fi * qr)
        tr, ti = tr - (gr * ur - gi * ui), ti - (gr * ui + gi * ur)
    pivots = jnp.where(diag, ar, 0.0)
    by_row = 1.0 / jnp.sqrt(jnp.sum(pivots, axis=1, keepdims=True))
    by_col = 1.0 / jnp.sqrt(jnp.sum(pivots, axis=0, keepdims=True))
    return mr * by_row, mi * by_row, tr * by_col, ti * by_col


def mixers(gram_real, gram_imag):
    width = gram_real.shape[0]

    def body(gr_ref, gi_ref, kr_ref, ki_ref):
        ar, ai = gr_ref[...], gi_ref[...]
        row = lax.broadcasted_iota(jnp.int32, ar.shape, 0)
        col = lax.broadcasted_iota(jnp.int32, ar.shape, 1)
        diag = row == col

        def ridge_of(real):
            total = jnp.sum(jnp.where(diag, real, 0.0), axis=0, keepdims=True)
            mean = jnp.sum(total, axis=1, keepdims=True) / width
            return ridge_scale * (mean + 1e-06)

        ridge = ridge_of(ar)
        ar = ar + jnp.where(diag, ridge, 0.0)
        mr, mi, tr, ti = inverse_factors(ar, ai)
        xr = jnp.zeros_like(ar)
        xi = jnp.zeros_like(ar)
        for m in range(width):
            lr, li = mr[:, m : m + 1], mi[:, m : m + 1]
            cr, ci = tr[m : m + 1], -ti[m : m + 1]
            xr = xr + (lr * cr - li * ci)
            xi = xi + (lr * ci + li * cr)
        br = jnp.where(diag, 1.0, 0.0) - ridge * xr
        bi = -ridge * xi
        br = br + jnp.where(diag, ridge_of(br), 0.0)
        sr, si, _, _ = inverse_factors(br, bi)
        kr = jnp.zeros_like(ar)
        ki = jnp.zeros_like(ar)
        for m in range(width):
            lr, li = sr[:, m : m + 1], si[:, m : m + 1]
            cr, ci = mr[m : m + 1], mi[m : m + 1]
            kr = kr + (lr * cr - li * ci)
            ki = ki + (lr * ci + li * cr)
        kr_ref[...] = kr
        ki_ref[...] = ki

    shape = jax.ShapeDtypeStruct(gram_real.shape, jnp.float32)
    return pl.pallas_call(body, out_shape=(shape, shape), name="factor")(gram_real, gram_imag)


def per_device(near_null, offsets, owner_slot):
    edge, _, _, vectors, comps, lanes = near_null.shape
    chiralities = 2
    half_c = comps // chiralities
    ta_size = lax.axis_size("ta")
    me = lax.axis_index("ta")
    direct = ta_size <= direct_limit
    slots = owner_slot.reshape(-1)
    count = slots.shape[0]
    per_peer = count // ta_size
    off_t = offsets[0]
    shift = offsets[3:4]

    before = from_behind(slots, "ta", 1)

    def places(slot_row):
        if not direct:
            return slot_row
        return ((slot_row // per_peer - me) % ta_size) * per_peer + slot_row % per_peer

    row_ids = jnp.arange(edge, dtype=jnp.int32)
    table = jnp.where((row_ids >= off_t)[:, None], places(slots)[None], places(before)[None])

    chunks = near_null.reshape(edge, edge, edge, vectors, chiralities, half_c, lanes)
    rows = vectors * half_c
    chunks = tuple(
        chunks[:, :, :, :, h].reshape(edge, edge, edge, rows, lanes) for h in range(chiralities)
    )

    def exchange(packed):
        packed = packed.reshape((ta_size, per_peer) + packed.shape[1:])
        if not direct:
            return lax.all_to_all(packed, "ta", split_axis=0, concat_axis=0, tiled=True)
        parts = [packed[:1]]
        for k in range(1, ta_size):
            parts.append(from_behind(packed[k : k + 1], "ta", k))
        return jnp.concatenate(parts, axis=0)

    owned = jnp.arange(count, dtype=jnp.int32)
    time_row = ((owned // per_peer) * edge)[:, None] + row_ids[None] + off_t
    time_row = time_row % (edge * ta_size)
    source = time_row // edge
    if direct:
        source = (me - source) % ta_size
    slot = jnp.broadcast_to((owned % per_peer)[:, None], (count, edge))
    where = (source, slot, time_row % edge)

    wide = 2 * vectors
    index = jnp.arange(2 * rows, dtype=jnp.int32)
    spread = (index[:, None] // half_c == jnp.arange(wide)[None]).astype(jnp.float32)
    gather = spread.T
    match = (index[:, None] % half_c == index[None] % half_c).astype(jnp.float32)

    norm_count = half_c * edge**4
    def travel(off_z, off_y):
        def run(data):
            results = []
            corner = None
            for d in data:
                near_y = d[:, off_z:, :off_y]
                if corner is not None:
                    near_y, corner = lax.optimization_barrier((near_y, corner))
                corner = from_behind(d[:, :off_z, :off_y], "gz", -1)
                side_y = from_behind(near_y, "gy", -1)
                side_z = from_behind(d[:, :off_z, off_y:], "gz", -1)
                corner = from_behind(corner, "gy", -1)
                left = jnp.concatenate([d[:, off_z:, off_y:], side_z], axis=1)
                right = jnp.concatenate([side_y, corner], axis=1)
                aligned = jnp.concatenate([left, right], axis=2)
                blocks = exchange(pack(aligned, shift, table, edge))
                results.append(blocks)
            early = [grams(b, where, spread, gather, match, norm_count, 1) for b in results[:-1]]
            return tuple(results), tuple(early)

        return run

    branches = [travel(i, j) for i in range(1, edge) for j in range(1, edge)]
    chunks, early = lax.switch((offsets[1] - 1) * (edge - 1) + (offsets[2] - 1), branches, chunks)

    result = None
    last = grams(
        chunks[-1], where, spread, gather, match, norm_count, batch_of(count)
    )
    for h, (blocks, gram) in enumerate(zip(chunks, early + (last,))):
        gram = gram.reshape(count, 2, vectors, 2, vectors).transpose(1, 3, 2, 4, 0)
        kr, ki = mixers(gram[0, 0] + gram[1, 1], gram[0, 1] - gram[1, 0])
        mixing = jnp.stack([jnp.stack([kr, ki]), jnp.stack([-ki, kr])])
        mixing = mixing.transpose(4, 0, 2, 1, 3).reshape(count, wide, wide)
        result = apply(blocks, where, mixing, spread, gather, match, h, result, chiralities)
    halves = edge**4 // LANES
    result = result.reshape(count, chiralities, vectors, half_c, halves, 2, LANES)
    result = result.transpose(0, 1, 2, 3, 5, 4, 6)
    return result.reshape(count, chiralities, vectors, half_c, 2, edge**4)


def solution(mesh):
    return jax.shard_map(
        per_device,
        mesh=mesh,
        in_specs=(P("ta", "gz", "gy", None, None, None), P(), P("ta", "gz", "gy", None)),
        out_specs=P(("ta", "gz", "gy"), None, None, None, None, None),
        check_vma=False,
    )
```
